32 devices in a mesh: occ: 4 (over z), vsec: 4 (over y, core), aux: 2 (over x).
Axes of the slice: x: 2, y: 2, z: 4, core: 2. Of those that a mesh axis runs over, the one named last changes fastest.
Arguments:
- amplitudes: bfloat16 [16, 1024, 1024], P(('occ', 'vsec'), 'aux'), may hold values from -0.005859375 to 0.005859375
- left_factor: bfloat16 [4096, 8, 1024], P('aux', 'vsec'), may hold values from -0.75 to 0.75
- right_factor: bfloat16 [4096, 8, 1024], P('aux', None, 'occ'), may hold values from -0.75 to 0.75
- other_terms: float32 [16, 8, 8], P(('occ', 'aux'), 'vsec'), may hold values from -10.4 to 10.4
Outputs:
- residual: float32 [16, 8, 8], P(('occ', 'aux'), 'vsec')
- residual_norm: float32 [], replicated
The draws below stay inside these ranges and needn't reach their ends.
All inputs are finite; a program needn't handle non-finite values.
Results may differ from the reference program's by a relative error of at most 0.002.
Values may be sent and summed in bfloat16 or wider, within the bound.
A program may use at most 192 MiB of HBM per device.

```python
import jax
import jax.numpy as jnp
from jax import lax

VIRT = 1024
NAUX = 4096
BWIN = 8
PAIRS = 16
AROWS = 8


def draw_other_terms(key, part):
    key_base = jax.random.fold_in(jax.random.fold_in(key, 17), 0)
    pair_pos = jnp.arange(PAIRS, dtype=jnp.float32) / max(PAIRS - 1, 1)
    row_pos = jnp.arange(AROWS, dtype=jnp.float32) / max(AROWS - 1, 1)
    rising = 0.5 * (12.0 ** (0.25 * pair_pos))[:, None, None] * (12.0 ** (0.25 * row_pos))[None, :, None]
    base = jax.random.normal(key_base, (PAIRS, AROWS, BWIN), jnp.float32)
    base = jnp.clip(base, -6.0, 6.0)
    return (base * rising).astype(jnp.float32)


def levels(rng, dims, cuts, least, top_value):
    gain, own = 1.0, jax.random.fold_in(rng, 6)
    for dim, parts in cuts:
        heights = jnp.exp(jax.random.uniform(jax.random.fold_in(own, dim), (parts,), jnp.float32, least / len(cuts), top_value / len(cuts)))
        gain = gain * jnp.repeat(heights, dims[dim] // parts).reshape([-1 if axis == dim else 1 for axis in range(len(dims))])
    return gain


def bell_draw(key, extent, width, reach, cuts=(), held_as=jnp.bfloat16):
    result = width * jax.random.normal(key, extent, jnp.float32)
    if cuts:
        result = result * levels(key, extent, cuts, -0.22, 0.18)
    return jnp.clip(result, -reach, reach).astype(held_as)


def setup_inputs(seed: int = 0) -> dict:
    seeds = jax.random.split(jax.random.key(seed), 5)
    amplitudes = bell_draw(seeds[0], (PAIRS, VIRT, VIRT), (VIRT * VIRT) ** -0.5, 0.005859375, ((0, 16), (1, 2)))
    left_factor = bell_draw(seeds[1], (NAUX, AROWS, VIRT), (NAUX ** 0.5) ** -0.5, 0.75, ((0, 2), (1, 4)))
    right_factor = bell_draw(seeds[2], (NAUX, BWIN, VIRT), (NAUX ** 0.5) ** -0.5, 0.75, ((0, 2), (2, 4)))
    other_terms = draw_other_terms(jax.random.fold_in(seeds[4], 71), 0)
    return {"amplitudes": amplitudes, "left_factor": left_factor, "right_factor": right_factor, "other_terms": other_terms}


def reference(amplitudes, left_factor, right_factor, other_terms):
    pairs_all = amplitudes.shape[0]
    virt_width = amplitudes.shape[1]
    aux_width = left_factor.shape[0]
    window = right_factor.shape[1]
    amp_flat = amplitudes.astype(jnp.float32).reshape(pairs_all, virt_width * virt_width)
    right_flat = right_factor.reshape(aux_width, window * virt_width)
    rows_first = jnp.transpose(left_factor, (1, 0, 2))

    def one_row(row_factor):
        integral = lax.dot_general(row_factor, right_flat, (((0,), (0,)), ((), ())), preferred_element_type=jnp.float32)
        rounded = lax.optimization_barrier(integral.astype(jnp.bfloat16))
        integral = rounded.astype(jnp.float32)
        integral = integral.reshape(virt_width, window, virt_width).transpose(0, 2, 1).reshape(virt_width * virt_width, window)
        return jnp.dot(amp_flat, integral, precision=lax.Precision.HIGHEST, preferred_element_type=jnp.float32)
    ladder = lax.map(one_row, rows_first)
    ladder = jnp.transpose(ladder, (1, 0, 2))
    residual = other_terms + ladder
    residual_norm = jnp.sqrt(jnp.sum(residual * residual))
    return (residual, residual_norm)
```

```python
import jax
import jax.numpy as jnp
from jax import lax
from jax.sharding import PartitionSpec as P


def pair_order(ladder, sec_count, occ_count, per_device, arow_count, window):
    ordered = ladder.reshape(sec_count, occ_count, per_device, arow_count, window)
    return jnp.transpose(ordered, (1, 0, 2, 3, 4)).reshape(
        sec_count * occ_count * per_device, arow_count, window
    )


def on_device(amplitudes, left_factor, right_factor, other_terms):
    occ_count = lax.axis_size("occ")
    sec_count = lax.axis_size("vsec")
    aux_rows, arow_count, virt_width = left_factor.shape
    window = right_factor.shape[1]
    slice_width = right_factor.shape[2]
    local_amps = lax.all_to_all(amplitudes, "occ", split_axis=2, concat_axis=0, tiled=True)
    pair_count = local_amps.shape[0]
    per_device = pair_count // occ_count
    amps = lax.all_gather(local_amps, ("vsec", "aux"), axis=0, tiled=False)
    amps = amps.reshape(sec_count, -1, pair_count, local_amps.shape[1], slice_width)
    partial_value = lax.dot_general(
        left_factor.reshape(aux_rows, arow_count * virt_width),
        right_factor.reshape(aux_rows, window * slice_width),
        (((0,), (0,)), ((), ())),
        preferred_element_type=jnp.float32,
    )
    high = partial_value.astype(jnp.bfloat16)
    low = (partial_value - high.astype(jnp.float32)).astype(jnp.bfloat16)

    def contract(half):
        half = half.reshape(arow_count, amps.shape[1], amps.shape[3], window, slice_width)
        return lax.dot_general(
            amps, half, (((1, 3, 4), (1, 2, 4)), ((), ())), preferred_element_type=jnp.float32
        )

    contrib = contract(high) + contract(low)
    ordered = pair_order(contrib, sec_count, occ_count, per_device, arow_count, window)
    summed = lax.psum_scatter(ordered, ("occ", "aux"), scatter_dimension=0, tiled=True)
    residual = other_terms + summed
    squares = lax.psum(jnp.sum(residual * residual), ("occ", "vsec", "aux"))
    return (residual, jnp.sqrt(squares))


def solution(mesh):
    placed = (
        P(("occ", "vsec"), "aux", None),
        P("aux", "vsec", None),
        P("aux", None, "occ"),
        P(("occ", "aux"), "vsec", None),
    )
    return jax.shard_map(
        on_device,
        mesh=mesh,
        in_specs=placed,
        out_specs=(P(("occ", "aux"), "vsec", None), P()),
        check_vma=False,
    )
```

```python
import functools

import jax
import jax.numpy as jnp
from jax import lax
from jax.experimental import pallas as pl
from jax.experimental.pallas import tpu as pltpu
from jax.sharding import PartitionSpec as P

MESH = pl.DeviceIdType.MESH
ROWS = 256
COLS = 512
GROUP = 16
LANES = 128


def ladder_kernel(
    sizes, amps_ref, left_hbm, right_hbm, other_ref, res_ref, norm_ref,
    tbuf, left, right, left_t, high, low, acc, parts, norms,
    send_sem, recv_sem, load_sem, part_send, part_recv, norm_send, norm_recv,
):
    n_occ, n_sec, n_aux = sizes
    n_hi = n_sec // 2
    occ, sec, aux = lax.axis_index("occ"), lax.axis_index("vsec"), lax.axis_index("aux")
    hi, core = sec // 2, sec % 2
    pairs, virt, dsl = tbuf.shape
    half = amps_ref.shape[1]
    wide = right.shape[1]
    window = wide // dsl
    rows_ab = high.shape[0]

    load_l = pltpu.make_async_copy(left_hbm, left, load_sem.at[0])
    load_r = pltpu.make_async_copy(right_hbm, right, load_sem.at[1])
    load_l.start()
    load_r.start()

    def turn(value, step, count):
        found = turns.get((id(value), step))
        return lax.rem(value + step + count, count) if found is None else found

    turns = {}
    for value, count in ((occ, n_occ), (sec, n_sec), (aux, n_aux), (hi, n_hi)):
        for step in range(1 - count, count):
            turns[id(value), step] = lax.rem(value + (step + count), count)
    pair_at = {
        (k, j, far): turn(occ, -k, n_occ) * n_sec + turn(hi, -j, n_hi) * 2 + (1 - core if far else core)
        for k in range(n_occ) for j in range(n_hi) for far in (False, True)
    }
    half_at = [pl.multiple_of(turn(aux, -i, n_aux) * half, half) for i in range(n_aux)]
    partner = hi * 2 + 1 - core
    hi_to = [turn(hi, j, n_hi) * 2 + core for j in range(n_hi)]

    group = [(k, i) for k in range(n_occ) for i in range(n_aux) if (k, i) != (0, 0)]
    barrier = pltpu.get_barrier_semaphore()
    for k, i in group:
        pl.semaphore_signal(
            barrier, inc=1, device_id={"occ": turn(occ, k, n_occ), "aux": turn(aux, i, n_aux)},
            device_id_type=MESH,
        )
    for j in range(1, n_sec):
        pl.semaphore_signal(
            barrier, inc=1, device_id={"vsec": turn(sec, j, n_sec)}, device_id_type=MESH
        )
    pl.semaphore_wait(barrier, len(group) + n_sec - 1)

    ids = {}
    numbers = [occ * 0 + number for number in range(n_occ * n_sec * n_aux)]

    def sem_of(key):
        return numbers[ids.setdefault(key, len(ids))]

    def slot(k, j, i, far=False):
        return tbuf.at[pair_at[k, j, far], pl.ds(half_at[i], half), :]

    sent = []

    def send(src, dst, key, target):
        number = sem_of(key)
        copy = pltpu.make_async_remote_copy(
            src_ref=src, dst_ref=dst, send_sem=send_sem.at[number], recv_sem=recv_sem.at[number],
            device_id=target, device_id_type=MESH,
        )
        copy.start()
        sent.append(copy)

    def arrive(key, k, j, i, far=False):
        number = sem_of(key)
        ref = slot(k, j, i, far)
        pltpu.make_async_remote_copy(
            src_ref=ref, dst_ref=ref, send_sem=send_sem.at[number], recv_sem=recv_sem.at[number],
            device_id={"vsec": partner}, device_id_type=MESH,
        ).wait_recv()

    def to_core(src, k, j, i):
        send(src, slot(k, j, i), ("c", k, j, i), {"vsec": partner})

    def to_hi(src, dst, key, j):
        send(src, dst, key, {"vsec": hi_to[j]})

    def to_aux(src, dst, key, i):
        send(src, dst, key, {"aux": turn(aux, i, n_aux)})

    def spread(src, k):
        dst = slot(k, 0, 0)
        for j in range(1, n_hi):
            to_hi(src, dst, ("y", k, j), j)
        for i in range(1, n_aux):
            to_aux(src, dst, ("x", k, i), i)
        to_core(src, k, 0, 0)

    def own_slice(step):
        return amps_ref.at[0, :, pl.ds(pl.multiple_of(turn(occ, step, n_occ) * dsl, dsl), dsl)]

    order = sorted(range(1, n_occ), key=lambda k: (min(k, n_occ - k), k))
    for k in order:
        send(own_slice(k), slot(0, 0, 0), ("z", k), {"occ": turn(occ, k, n_occ)})
    spread(own_slice(0), 0)
    keep = pltpu.make_async_copy(own_slice(0), slot(0, 0, 0), load_sem.at[2])
    keep.start()

    def z_event(k):
        arrive(("z", k), k, 0, 0)
        spread(slot(k, 0, 0), k)

    def yx_event(k, turn_no):
        for j in range(1, n_hi):
            arrive(("y", k, j), k, j, 0)
            ref = slot(k, j, 0)
            if turn_no % 2 == 0:
                for i in range(1, n_aux):
                    to_aux(ref, ref, ("d", k, j, i), i)
            to_core(ref, k, j, 0)
        for i in range(1, n_aux):
            arrive(("x", k, i), k, 0, i)
            ref = slot(k, 0, i)
            if turn_no % 2 == 1:
                for j in range(1, n_hi):
                    to_hi(ref, ref, ("d", k, j, i), j)
            to_core(ref, k, 0, i)

    def d_event(k):
        for j in range(1, n_hi):
            for i in range(1, n_aux):
                arrive(("d", k, j, i), k, j, i)
                to_core(slot(k, j, i), k, j, i)

    every = [0] + order
    events = []
    for t, k in enumerate(every):
        if t + 1 < n_occ:
            events.append(functools.partial(z_event, every[t + 1]))
        events.append(functools.partial(yx_event, k, t))
        if t >= 1:
            events.append(functools.partial(d_event, every[t - 1]))
    events.append(functools.partial(d_event, every[-1]))

    load_l.wait()
    load_r.wait()
    n_m, n_n = left.shape[1] // ROWS, wide // COLS
    per_arow = virt // ROWS
    spots = n_m * n_n
    first, pace = 4, max(1, (spots - 4) // (len(events) + 1))
    at_spot = {}
    for e, event in enumerate(events):
        place = first + e * pace
        at_spot.setdefault(place if place < spots else None, []).append(event)

    def block(m, carry):
        left_t[...] = left[:, pl.ds(pl.multiple_of(m * ROWS, ROWS), ROWS)].T
        arow = m // per_arow
        c_at = pl.multiple_of((m % per_arow) * ROWS, ROWS)
        for n in range(n_n):
            value = jnp.dot(
                left_t[...], right[:, n * COLS:(n + 1) * COLS], preferred_element_type=jnp.float32
            )
            top = value.astype(jnp.bfloat16)
            rest = (value - top.astype(jnp.float32)).astype(jnp.bfloat16)
            for b in range(COLS // dsl):
                at = arow * window + n * (COLS // dsl) + b
                high[at, pl.ds(c_at, ROWS), :] = top[:, b * dsl:(b + 1) * dsl]
                low[at, pl.ds(c_at, ROWS), :] = rest[:, b * dsl:(b + 1) * dsl]
            for place, todo in at_spot.items():
                if place is not None and place % n_n == n:
                    @pl.when(m == place // n_n)
                    def _(todo=todo):
                        for event in todo:
                            event()
        return carry

    lax.fori_loop(0, n_m, block, 0)
    for event in at_spot.get(None, []):
        event()
    keep.wait()
    for k in every:
        for j in range(n_hi):
            for i in range(n_aux):
                arrive(("c", k, j, i), k, j, i, True)

    span = GROUP * 4
    rows = min(pairs, 16)
    for p in range(0, pairs, rows):
        acc[...] = jnp.zeros_like(acc)

        def contract(g, carry):
            def gathered(ref, lead, count):
                return jnp.concatenate(
                    [
                        ref[pl.ds(lead, count), pl.ds(pl.multiple_of(g * span + q * GROUP, GROUP), GROUP), :]
                        .reshape(count * GROUP, dsl)
                        for q in range(span // GROUP)
                    ],
                    axis=1,
                )

            amp = gathered(tbuf, p, rows)
            dims = (((1,), (1,)), ((), ()))
            acc[...] += lax.dot_general(
                amp, gathered(high, 0, rows_ab), dims, preferred_element_type=jnp.float32
            ) + lax.dot_general(
                amp, gathered(low, 0, rows_ab), dims, preferred_element_type=jnp.float32
            )
            return carry

        lax.fori_loop(0, virt // span, contract, 0)
        shape = acc.shape
        row = lax.broadcasted_iota(jnp.int32, shape, 0) % GROUP
        col = lax.broadcasted_iota(jnp.int32, shape, 1) % GROUP
        diag = jnp.where(row == col, acc[...], 0.0)
        diag = jnp.sum(diag.reshape(rows, GROUP, shape[1]), axis=1)
        pick = (
            lax.broadcasted_iota(jnp.int32, (shape[1], LANES), 0) // GROUP
            == lax.broadcasted_iota(jnp.int32, (shape[1], LANES), 1)
        ).astype(jnp.float32)
        parts[0, pl.ds(p, rows), :] = jnp.dot(
            diag, pick, precision=lax.Precision.HIGHEST, preferred_element_type=jnp.float32
        )

    per = other_ref.shape[0]
    mine = occ * n_aux + aux
    base = mine * per
    row = lax.broadcasted_iota(jnp.int32, (pairs, LANES), 0)
    whole = parts[0]
    for r in range(per):
        whole = whole + jnp.where(row == base + r, other_ref[r:r + 1, :], 0.0)
    members = n_occ * n_aux
    parts[1 + mine] = whole
    started = []
    for number, (k, i) in enumerate(group):
        copy = pltpu.make_async_remote_copy(
            src_ref=parts.at[1 + mine], dst_ref=parts.at[1 + mine],
            send_sem=part_send.at[number], recv_sem=part_recv.at[number],
            device_id={"occ": turn(occ, k, n_occ), "aux": turn(aux, i, n_aux)}, device_id_type=MESH,
        )
        copy.start()
        started.append(copy)
    assert len(sent) == len(numbers) - 1
    for copy in sent:
        copy.wait_send()
    for number, (k, i) in enumerate(group):
        ref = parts.at[1 + turn(occ, -k, n_occ) * n_aux + turn(aux, -i, n_aux)]
        pltpu.make_async_remote_copy(
            src_ref=ref, dst_ref=ref, send_sem=part_send.at[number], recv_sem=part_recv.at[number],
            device_id={"occ": turn(occ, k, n_occ), "aux": turn(aux, i, n_aux)}, device_id_type=MESH,
        ).wait_recv()
    total = parts[1]
    for g in range(1, members):
        total = total + parts[1 + g]
    squares = jnp.sum(jnp.sum(total * total, axis=0, keepdims=True), axis=1, keepdims=True)
    norms[sec] = jnp.broadcast_to(squares, (1, LANES))
    for j in range(1, n_sec):
        copy = pltpu.make_async_remote_copy(
            src_ref=norms.at[sec], dst_ref=norms.at[sec],
            send_sem=norm_send.at[j], recv_sem=norm_recv.at[j],
            device_id={"vsec": turn(sec, j, n_sec)}, device_id_type=MESH,
        )
        copy.start()
        started.append(copy)
    for r in range(per):
        res_ref[r:r + 1, :] = jnp.sum(
            jnp.where(row == base + r, total, 0.0), axis=0, keepdims=True
        )
    for j in range(1, n_sec):
        ref = norms.at[turn(sec, -j, n_sec)]
        pltpu.make_async_remote_copy(
            src_ref=ref, dst_ref=ref, send_sem=norm_send.at[j], recv_sem=norm_recv.at[j],
            device_id={"vsec": turn(sec, j, n_sec)}, device_id_type=MESH,
        ).wait_recv()
    squares = norms[0]
    for j in range(1, n_sec):
        squares = squares + norms[j]
    norm_ref[...] = jnp.sqrt(squares)
    for copy in started:
        copy.wait_send()


def on_device(sizes, amplitudes, left_factor, right_factor, other_terms):
    n_occ, n_sec, n_aux = sizes
    aux_rows, arow_count, virt = left_factor.shape
    window, dsl = right_factor.shape[1:]
    pairs = n_occ * n_sec
    per = other_terms.shape[0]
    ab = arow_count * window
    left = left_factor.reshape(aux_rows, arow_count * virt)
    right = right_factor.reshape(aux_rows, window * dsl)
    other = jnp.pad(other_terms.reshape(per, ab), ((0, 0), (0, LANES - ab)))
    copies = pairs * n_aux
    members = n_occ * n_aux
    rows = min(pairs, 16)
    dma = pltpu.SemaphoreType.DMA
    vmem = pl.BlockSpec(memory_space=pltpu.VMEM)
    anywhere = pl.BlockSpec(memory_space=pl.ANY)
    res, norm = pl.pallas_call(
        functools.partial(ladder_kernel, sizes),
        out_shape=(
            jax.ShapeDtypeStruct((per, LANES), jnp.float32),
            jax.ShapeDtypeStruct((1, LANES), jnp.float32),
        ),
        in_specs=[vmem, anywhere, anywhere, vmem],
        out_specs=(vmem, vmem),
        scratch_shapes=[
            pltpu.VMEM((pairs, virt, dsl), jnp.bfloat16),
            pltpu.VMEM(left.shape, jnp.bfloat16),
            pltpu.VMEM(right.shape, jnp.bfloat16),
            pltpu.VMEM((ROWS, aux_rows), jnp.bfloat16),
            pltpu.VMEM((ab, virt, dsl), jnp.bfloat16),
            pltpu.VMEM((ab, virt, dsl), jnp.bfloat16),
            pltpu.VMEM((rows * GROUP, ab * GROUP), jnp.float32),
            pltpu.VMEM((1 + members, pairs, LANES), jnp.float32),
            pltpu.VMEM((n_sec, 1, LANES), jnp.float32),
            dma((copies,)), dma((copies,)), dma((3,)),
            dma((members,)), dma((members,)), dma((n_sec,)), dma((n_sec,)),
        ],
        compiler_params=pltpu.CompilerParams(
            collective_id=0, has_side_effects=True, vmem_limit_bytes=64000 * 1024
        ),
    )(amplitudes, left, right, other)
    return res[:, :ab].reshape(other_terms.shape), norm[0, 0]


def solution(mesh):
    placed = (
        P(("occ", "vsec"), "aux", None),
        P("aux", "vsec", None),
        P("aux", None, "occ"),
        P(("occ", "aux"), "vsec", None),
    )
    sizes = (mesh.shape["occ"], mesh.shape["vsec"], mesh.shape["aux"])
    return jax.shard_map(
        functools.partial(on_device, sizes),
        mesh=mesh,
        in_specs=placed,
        out_specs=(P(("occ", "aux"), "vsec", None), P()),
        check_vma=False,
    )
```

```python
import functools

import jax
import jax.numpy as jnp
from jax import lax
from jax.experimental import pallas as pl
from jax.experimental.pallas import tpu as pltpu
from jax.sharding import PartitionSpec as P

MESH = pl.DeviceIdType.MESH
ROWS = 256
COLS = 512
GROUP = 16
LANES = 128


def ladder_kernel(
    sizes, amps_ref, left_hbm, right_hbm, other_ref, res_ref, norm_ref,
    tbuf, left, right_in, right, left_t, high, low, acc, parts, norms,
    send_sem, recv_sem, load_sem, part_send, part_recv, norm_send, norm_recv,
):
    n_occ, n_sec, n_aux = sizes
    n_hi = n_sec // 2
    occ, sec, aux = lax.axis_index("occ"), lax.axis_index("vsec"), lax.axis_index("aux")
    hi, core = sec // 2, sec % 2
    pairs, virt, dsl = tbuf.shape
    half = amps_ref.shape[1]
    wide = right.shape[1]
    window = wide // dsl
    rows_ab = high.shape[0]

    load_l = pltpu.make_async_copy(left_hbm, left, load_sem.at[0])
    load_r = pltpu.make_async_copy(right_hbm, right_in, load_sem.at[1])
    load_l.start()
    load_r.start()

    def turn(value, step, count):
        found = turns.get((id(value), step))
        return lax.rem(value + step + count, count) if found is None else found

    turns = {}
    for value, count in ((occ, n_occ), (sec, n_sec), (aux, n_aux), (hi, n_hi)):
        for step in range(1 - count, count):
            turns[id(value), step] = lax.rem(value + (step + count), count)
    pair_at = {
        (k, j, far): turn(occ, -k, n_occ) * n_sec + turn(hi, -j, n_hi) * 2 + (1 - core if far else core)
        for k in range(n_occ) for j in range(n_hi) for far in (False, True)
    }
    half_at = [pl.multiple_of(turn(aux, -i, n_aux) * half, half) for i in range(n_aux)]
    partner = hi * 2 + 1 - core
    hi_to = [turn(hi, j, n_hi) * 2 + core for j in range(n_hi)]

    group = [(k, i) for k in range(n_occ) for i in range(n_aux) if (k, i) != (0, 0)]
    barrier = pltpu.get_barrier_semaphore()
    for k, i in group:
        pl.semaphore_signal(
            barrier, inc=1, device_id={"occ": turn(occ, k, n_occ), "aux": turn(aux, i, n_aux)},
            device_id_type=MESH,
        )
    for j in range(1, n_sec):
        pl.semaphore_signal(
            barrier, inc=1, device_id={"vsec": turn(sec, j, n_sec)}, device_id_type=MESH
        )
    pl.semaphore_wait(barrier, len(group) + n_sec - 1)

    ids = {}
    numbers = [occ * 0 + number for number in range(n_occ * n_sec * n_aux)]

    def sem_of(key):
        return numbers[ids.setdefault(key, len(ids))]

    def slot(k, j, i, far=False):
        return tbuf.at[pair_at[k, j, far], pl.ds(half_at[i], half), :]

    sent = []

    def send(src, dst, key, target):
        number = sem_of(key)
        copy = pltpu.make_async_remote_copy(
            src_ref=src, dst_ref=dst, send_sem=send_sem.at[number], recv_sem=recv_sem.at[number],
            device_id=target, device_id_type=MESH,
        )
        copy.start()
        sent.append(copy)

    def arrive(key, k, j, i, far=False):
        number = sem_of(key)
        ref = slot(k, j, i, far)
        pltpu.make_async_remote_copy(
            src_ref=ref, dst_ref=ref, send_sem=send_sem.at[number], recv_sem=recv_sem.at[number],
            device_id={"vsec": partner}, device_id_type=MESH,
        ).wait_recv()

    def to_core(src, k, j, i):
        send(src, slot(k, j, i), ("c", k, j, i), {"vsec": partner})

    def to_hi(src, dst, key, j):
        send(src, dst, key, {"vsec": hi_to[j]})

    def to_aux(src, dst, key, i):
        send(src, dst, key, {"aux": turn(aux, i, n_aux)})

    def spread(src, k):
        dst = slot(k, 0, 0)
        for j in range(1, n_hi):
            to_hi(src, dst, ("y", k, j), j)
        for i in range(1, n_aux):
            to_aux(src, dst, ("x", k, i), i)
        to_core(src, k, 0, 0)

    def own_slice(step):
        return amps_ref.at[0, :, pl.ds(pl.multiple_of(turn(occ, step, n_occ) * dsl, dsl), dsl)]

    order = sorted(range(1, n_occ), key=lambda k: (min(k, n_occ - k), k))
    for k in order:
        send(own_slice(k), slot(0, 0, 0), ("z", k), {"occ": turn(occ, k, n_occ)})
    spread(own_slice(0), 0)
    keep = pltpu.make_async_copy(own_slice(0), slot(0, 0, 0), load_sem.at[2])
    keep.start()

    def z_event(k):
        arrive(("z", k), k, 0, 0)
        spread(slot(k, 0, 0), k)

    def yx_event(k, turn_no):
        for j in range(1, n_hi):
            arrive(("y", k, j), k, j, 0)
            ref = slot(k, j, 0)
            if turn_no % 2 == 0:
                for i in range(1, n_aux):
                    to_aux(ref, ref, ("d", k, j, i), i)
            to_core(ref, k, j, 0)
        for i in range(1, n_aux):
            arrive(("x", k, i), k, 0, i)
            ref = slot(k, 0, i)
            if turn_no % 2 == 1:
                for j in range(1, n_hi):
                    to_hi(ref, ref, ("d", k, j, i), j)
            to_core(ref, k, 0, i)

    def d_event(k):
        for j in range(1, n_hi):
            for i in range(1, n_aux):
                arrive(("d", k, j, i), k, j, i)
                to_core(slot(k, j, i), k, j, i)

    every = [0] + order
    events = []
    for t, k in enumerate(every):
        if t + 1 < n_occ:
            events.append(functools.partial(z_event, every[t + 1]))
        events.append(functools.partial(yx_event, k, t))
        if t >= 1:
            events.append(functools.partial(d_event, every[t - 1]))
    events.append(functools.partial(d_event, every[-1]))

    load_l.wait()
    load_r.wait()
    early = 3
    for event in events[:early]:
        event()
    events = events[early:]
    aux_rows, arow_count = left.shape[:2]
    n_m, n_col = virt // ROWS, wide // COLS
    n_n = arow_count * n_col
    spots = n_m * n_n

    def flatten(step, carry):
        at = pl.ds(pl.multiple_of(step * ROWS, ROWS), ROWS)
        for b in range(window):
            right[at, b * dsl:(b + 1) * dsl] = right_in[at, b, :]
        return carry

    lax.fori_loop(0, aux_rows // ROWS, flatten, 0)
    first, pace = 0, max(1, spots // max(1, len(events)))
    at_spot = {}
    for e, event in enumerate(events):
        place = first + e * pace
        at_spot.setdefault(place if place < spots else None, []).append(event)

    def block(m, carry):
        c_at = pl.multiple_of(m * ROWS, ROWS)
        for n in range(n_n):
            arow, col = n // n_col, n % n_col
            if col == 0:
                left_t[...] = left[:, arow, pl.ds(c_at, ROWS)].T
            value = jnp.dot(
                left_t[...], right[:, col * COLS:(col + 1) * COLS], preferred_element_type=jnp.float32
            )
            top = value.astype(jnp.bfloat16)
            rest = (value - top.astype(jnp.float32)).astype(jnp.bfloat16)
            for b in range(COLS // dsl):
                at = arow * window + col * (COLS // dsl) + b
                high[at, pl.ds(c_at, ROWS), :] = top[:, b * dsl:(b + 1) * dsl]
                low[at, pl.ds(c_at, ROWS), :] = rest[:, b * dsl:(b + 1) * dsl]
            for place, todo in at_spot.items():
                if place is not None and place % n_n == n:
                    @pl.when(m == place // n_n)
                    def _(todo=todo):
                        for event in todo:
                            event()
        return carry

    lax.fori_loop(0, n_m, block, 0)
    for event in at_spot.get(None, []):
        event()
    keep.wait()
    for k in every:
        for j in range(n_hi):
            for i in range(n_aux):
                arrive(("c", k, j, i), k, j, i, True)

    span = GROUP * 4
    rows = min(pairs, 16)
    for p in range(0, pairs, rows):
        acc[...] = jnp.zeros_like(acc)

        def contract(g, carry):
            def gathered(ref, lead, count):
                return jnp.concatenate(
                    [
                        ref[pl.ds(lead, count), pl.ds(pl.multiple_of(g * span + q * GROUP, GROUP), GROUP), :]
                        .reshape(count * GROUP, dsl)
                        for q in range(span // GROUP)
                    ],
                    axis=1,
                )

            amp = gathered(tbuf, p, rows)
            dims = (((1,), (1,)), ((), ()))
            acc[...] += lax.dot_general(
                amp, gathered(high, 0, rows_ab), dims, preferred_element_type=jnp.float32
            ) + lax.dot_general(
                amp, gathered(low, 0, rows_ab), dims, preferred_element_type=jnp.float32
            )
            return carry

        lax.fori_loop(0, virt // span, contract, 0)
        shape = acc.shape
        row = lax.broadcasted_iota(jnp.int32, shape, 0) % GROUP
        col = lax.broadcasted_iota(jnp.int32, shape, 1) % GROUP
        diag = jnp.where(row == col, acc[...], 0.0)
        diag = jnp.sum(diag.reshape(rows, GROUP, shape[1]), axis=1)
        pick = (
            lax.broadcasted_iota(jnp.int32, (shape[1], LANES), 0) // GROUP
            == lax.broadcasted_iota(jnp.int32, (shape[1], LANES), 1)
        ).astype(jnp.float32)
        parts[0, pl.ds(p, rows), :] = jnp.dot(
            diag, pick, precision=lax.Precision.HIGHEST, preferred_element_type=jnp.float32
        )

    per = other_ref.shape[0]
    mine = occ * n_aux + aux
    base = mine * per
    row = lax.broadcasted_iota(jnp.int32, (pairs, LANES), 0)
    whole = parts[0]
    for r in range(per):
        whole = whole + jnp.where(row == base + r, other_ref[r:r + 1, :], 0.0)
    members = n_occ * n_aux
    parts[1 + mine] = whole
    started = []
    for number, (k, i) in enumerate(group):
        copy = pltpu.make_async_remote_copy(
            src_ref=parts.at[1 + mine], dst_ref=parts.at[1 + mine],
            send_sem=part_send.at[number], recv_sem=part_recv.at[number],
            device_id={"occ": turn(occ, k, n_occ), "aux": turn(aux, i, n_aux)}, device_id_type=MESH,
        )
        copy.start()
        started.append(copy)
    assert len(sent) == len(numbers) - 1
    for copy in sent:
        copy.wait_send()
    for number, (k, i) in enumerate(group):
        ref = parts.at[1 + turn(occ, -k, n_occ) * n_aux + turn(aux, -i, n_aux)]
        pltpu.make_async_remote_copy(
            src_ref=ref, dst_ref=ref, send_sem=part_send.at[number], recv_sem=part_recv.at[number],
            device_id={"occ": turn(occ, k, n_occ), "aux": turn(aux, i, n_aux)}, device_id_type=MESH,
        ).wait_recv()
    total = parts[1]
    for g in range(1, members):
        total = total + parts[1 + g]
    squares = jnp.sum(jnp.sum(total * total, axis=0, keepdims=True), axis=1, keepdims=True)
    norms[sec] = jnp.broadcast_to(squares, (1, LANES))
    for j in range(1, n_sec):
        copy = pltpu.make_async_remote_copy(
            src_ref=norms.at[sec], dst_ref=norms.at[sec],
            send_sem=norm_send.at[j], recv_sem=norm_recv.at[j],
            device_id={"vsec": turn(sec, j, n_sec)}, device_id_type=MESH,
        )
        copy.start()
        started.append(copy)
    for r in range(per):
        res_ref[r:r + 1, :] = jnp.sum(
            jnp.where(row == base + r, total, 0.0), axis=0, keepdims=True
        )
    for j in range(1, n_sec):
        ref = norms.at[turn(sec, -j, n_sec)]
        pltpu.make_async_remote_copy(
            src_ref=ref, dst_ref=ref, send_sem=norm_send.at[j], recv_sem=norm_recv.at[j],
            device_id={"vsec": turn(sec, j, n_sec)}, device_id_type=MESH,
        ).wait_recv()
    squares = norms[0]
    for j in range(1, n_sec):
        squares = squares + norms[j]
    norm_ref[...] = jnp.sqrt(squares)
    for copy in started:
        copy.wait_send()


def on_device(sizes, amplitudes, left_factor, right_factor, other_terms):
    n_occ, n_sec, n_aux = sizes
    aux_rows, arow_count, virt = left_factor.shape
    window, dsl = right_factor.shape[1:]
    pairs = n_occ * n_sec
    per = other_terms.shape[0]
    ab = arow_count * window
    other = jnp.pad(other_terms.reshape(per, ab), ((0, 0), (0, LANES - ab)))
    copies = pairs * n_aux
    members = n_occ * n_aux
    rows = min(pairs, 16)
    dma = pltpu.SemaphoreType.DMA
    vmem = pl.BlockSpec(memory_space=pltpu.VMEM)
    anywhere = pl.BlockSpec(memory_space=pl.ANY)
    res, norm = pl.pallas_call(
        functools.partial(ladder_kernel, sizes),
        out_shape=(
            jax.ShapeDtypeStruct((per, LANES), jnp.float32),
            jax.ShapeDtypeStruct((1, LANES), jnp.float32),
        ),
        in_specs=[vmem, anywhere, anywhere, vmem],
        out_specs=(vmem, vmem),
        scratch_shapes=[
            pltpu.VMEM((pairs, virt, dsl), jnp.bfloat16),
            pltpu.VMEM(left_factor.shape, jnp.bfloat16),
            pltpu.VMEM(right_factor.shape, jnp.bfloat16),
            pltpu.VMEM((aux_rows, window * dsl), jnp.bfloat16),
            pltpu.VMEM((ROWS, aux_rows), jnp.bfloat16),
            pltpu.VMEM((ab, virt, dsl), jnp.bfloat16),
            pltpu.VMEM((ab, virt, dsl), jnp.bfloat16),
            pltpu.VMEM((rows * GROUP, ab * GROUP), jnp.float32),
            pltpu.VMEM((1 + members, pairs, LANES), jnp.float32),
            pltpu.VMEM((n_sec, 1, LANES), jnp.float32),
            dma((copies,)), dma((copies,)), dma((3,)),
            dma((members,)), dma((members,)), dma((n_sec,)), dma((n_sec,)),
        ],
        compiler_params=pltpu.CompilerParams(
            collective_id=0, has_side_effects=True, vmem_limit_bytes=64000 * 1024
        ),
    )(amplitudes, left_factor, right_factor, other)
    return res[:, :ab].reshape(other_terms.shape), norm[0, 0]


def solution(mesh):
    placed = (
        P(("occ", "vsec"), "aux", None),
        P("aux", "vsec", None),
        P("aux", None, "occ"),
        P(("occ", "aux"), "vsec", None),
    )
    sizes = (mesh.shape["occ"], mesh.shape["vsec"], mesh.shape["aux"])
    return jax.shard_map(
        functools.partial(on_device, sizes),
        mesh=mesh,
        in_specs=placed,
        out_specs=(P(("occ", "aux"), "vsec", None), P()),
        check_vma=False,
    )
```
